32 devices in a mesh: blk: 16 (over z, y, x), ch: 2 (over core).
Axes of the slice: x: 2, y: 2, z: 4, core: 2. Of those that a mesh axis runs over, the one named last changes fastest.
Arguments:
- features: bfloat16 [4096, 128], P('blk'), may hold values from -6 to 6
- out_grad: bfloat16 [4096, 256], P('blk', 'ch'), may hold values from -6 to 6
- weight: bfloat16 [256, 256], P('ch'), may hold values from -0.375 to 0.375
- neighbour_slot: int32 [4096, 20], P('blk'), may hold values from 0 to 2303
- argmax_edge: int32 [4096, 256], P('blk', 'ch'), may hold values from 0 to 19
Outputs:
- feature_grad: float32 [4096, 128], P('blk')
- weight_grad: float32 [256, 256], P('ch')
The draws below stay inside these ranges and needn't reach their ends.
Inputs may be any that keep to these rules, and one draw needn't show every extreme that they name: `neighbour_slot`: slot s stands for row s mod 256 of the block s // 256 - 4 places away from the point's own block around the cycle.
All inputs are finite; a program needn't handle non-finite values.
Results may differ from the reference program's by a relative error of at most 0.0044.
Values may be sent and summed in bfloat16 or wider, within the bound.
No kernel may reach another device: no remote copies, remote signals or barrier semaphores. Data moves between devices by JAX's collectives and lax.ppermute only.
A program may use at most 64 MiB of HBM per device.

```python
import jax
import jax.numpy as jnp
from jax import lax

CIN = 128
COUT = 256
KNN = 20
REACH = 4
PTS = 256
POINTS = 4096
N_BLK = 16


def plant(drawn, key, low, largest):
    longest = drawn.shape.index(max(drawn.shape))
    spots = []
    for shift in (0, 1):
        where = [jax.random.randint(jax.random.fold_in(key, axis), (), 0, length) for axis, length in enumerate(drawn.shape)]
        where[longest] = (where[longest] + shift) % drawn.shape[longest]
        spots.append(tuple(where))
    return drawn.at[spots[0]].set(low).at[spots[1]].set(largest)


def steps_of(stream_key, dims, cuts, low, high):
    factor_of = 1.0
    for axis_at, blocks in cuts:
        draws = jax.random.uniform(jax.random.fold_in(jax.random.fold_in(stream_key, 6), axis_at), (blocks,), jnp.float32, low / len(cuts), high / len(cuts))
        factor_of = factor_of * jnp.repeat(jnp.exp(draws), dims[axis_at] // blocks).reshape((-1,) + (1,) * (len(dims) - 1 - axis_at))
    return factor_of


def noise(own_key, shape, width, bound, shards=(), kind=jnp.bfloat16):
    level = steps_of(own_key, shape, shards, -0.22, 0.18) if shards else 1.0
    result = jax.random.normal(own_key, shape, jnp.float32) * width * level
    return jnp.minimum(jnp.maximum(result, -bound), bound).astype(kind)


def setup_inputs(seed: int = 0) -> dict:
    keys = jax.random.split(jax.random.key(seed), 6)
    features = noise(keys[0], (POINTS, CIN), 1.0, 6.0, ((0, 16),))
    out_grad = noise(keys[1], (POINTS, COUT), 1.0, 6.0, ((0, 16), (1, 2)))
    weight = noise(keys[2], (COUT, 2 * CIN), (2 * CIN) ** -0.5, 0.375, ((0, 2),))
    neighbour_slot = plant(jax.random.randint(keys[3], (POINTS, KNN), 0, (2 * REACH + 1) * PTS), jax.random.fold_in(keys[3], 1), 0, ((2 * REACH + 1) * PTS) - 1).astype(jnp.int32)
    argmax_edge = plant(jax.random.randint(keys[4], (POINTS, COUT), 0, KNN), jax.random.fold_in(keys[4], 1), 0, KNN - 1).astype(jnp.int32)
    return dict(features=features, out_grad=out_grad, weight=weight, neighbour_slot=neighbour_slot, argmax_edge=argmax_edge)


def silu_slope(pre):
    sig = jax.nn.sigmoid(pre)
    return sig * (1.0 + pre * (1.0 - sig))


def reference(features, out_grad, weight, neighbour_slot, argmax_edge):
    in_width = features.shape[1]
    w_self = weight[:, :in_width]
    w_nbr = weight[:, in_width:]
    w_diff = (w_self.astype(jnp.float32) - w_nbr.astype(jnp.float32)).astype(jnp.bfloat16)
    offsets = jnp.arange(2 * REACH + 1, dtype=jnp.int32) - REACH
    row_ids = jnp.arange(PTS, dtype=jnp.int32)
    edge_ids = jnp.arange(KNN, dtype=jnp.int32)
    window_rows = (2 * REACH + 1) * PTS

    def per_block(running, block_id):
        grad_acc, weight_acc = running
        owners = (block_id + offsets) % N_BLK
        rows = (owners[:, None] * PTS + row_ids[None, :]).reshape(-1).astype(jnp.int32)
        window = features[rows]
        start = (block_id * PTS).astype(jnp.int32)
        own_rows = lax.dynamic_slice_in_dim(features, start, PTS, 0)
        own_grad = lax.dynamic_slice_in_dim(out_grad, start, PTS, 0)
        slots = lax.dynamic_slice_in_dim(neighbour_slot, start, PTS, 0)
        picks = lax.dynamic_slice_in_dim(argmax_edge, start, PTS, 0)
        self_term = jnp.dot(own_rows, w_diff.T, preferred_element_type=jnp.float32)
        values = jnp.dot(window, w_nbr.T, preferred_element_type=jnp.float32)
        pre = self_term[:, None, :] + values[slots]
        keep = picks[:, None, :] == edge_ids[None, :, None]
        edge_grad = jnp.where(keep, own_grad.astype(jnp.float32)[:, None, :] * silu_slope(pre), 0.0).astype(jnp.bfloat16)
        grad_sum = jnp.sum(edge_grad.astype(jnp.float32), axis=1).astype(jnp.bfloat16)
        gathered = jax.ops.segment_sum(edge_grad.reshape(-1, edge_grad.shape[2]).astype(jnp.float32), slots.reshape(-1), num_segments=window_rows).astype(jnp.bfloat16)
        contrib = jnp.dot(gathered, w_nbr, preferred_element_type=jnp.float32)
        self_grad = jnp.dot(grad_sum, w_diff, preferred_element_type=jnp.float32)
        contrib = contrib.at[REACH * PTS:(REACH + 1) * PTS].add(self_grad)
        grad_acc = grad_acc.at[rows].add(contrib)
        own_part = lax.dot_general(grad_sum, own_rows, (((0,), (0,)), ((), ())), preferred_element_type=jnp.float32)
        nbr_total = lax.dot_general(gathered, window, (((0,), (0,)), ((), ())), preferred_element_type=jnp.float32)
        weight_acc = weight_acc + jnp.concatenate([own_part, nbr_total - own_part], axis=1)
        return (grad_acc, weight_acc), None

    start_state = (jnp.zeros((POINTS, in_width), jnp.float32), jnp.zeros(weight.shape, jnp.float32))
    (grad_acc, weight_acc), _ = lax.scan(per_block, start_state, jnp.arange(N_BLK, dtype=jnp.int32))
    return grad_acc, weight_acc * (POINTS ** -0.5)
```

```python
import functools

import jax
import jax.numpy as jnp
from jax import lax
from jax.experimental import pallas as pl
from jax.experimental.pallas import tpu as pltpu
from jax.sharding import PartitionSpec as P

REACH = 4
LANES = 128
BF16 = jnp.bfloat16
F32 = jnp.float32


def dot(a, b, da, db):
    return lax.dot_general(a, b, (((da,), (db,)), ((), ())), preferred_element_type=F32)


def local_kernel(
    ch_ref, own_ref, mine_ref, other_ref, wdiff_ref, wnbr_ref, slot_ref, pick_ref, grad_ref,
    keep_ref, give_ref, self_ref, terms_ref,
    values, low, high, edge, spread, contrib,
):
    points = own_ref.shape[0]
    columns, width = wnbr_ref.shape
    neighbours = slot_ref.shape[0]
    tiles = values.shape[0]
    per_block = points // LANES
    ch = ch_ref[0]
    w_nbr = wnbr_ref[...]
    w_diff = wdiff_ref[...]

    def window_tile(tile):
        block, part = tile // per_block, tile % per_block
        offset = block - REACH
        if offset == 0:
            return own_ref[pl.ds(part * LANES, LANES), :]
        row = (abs(offset) - 1) * points + part * LANES
        side = ch if offset < 0 else 1 - ch
        return jnp.where(
            side == 0, mine_ref[pl.ds(row, LANES), :], other_ref[pl.ds(row, LANES), :]
        )

    for tile in range(tiles):
        values[tile] = dot(w_nbr, window_tile(tile), 1, 1)

    for part in range(per_block):
        cols = pl.ds(part * LANES, LANES)
        pick = pick_ref[:, cols]
        slot = jnp.zeros_like(pick)
        for k in range(neighbours):
            slot = jnp.where(pick == k, slot_ref[pl.ds(k, 1), cols], slot)
        lo = slot & (LANES - 1)
        hi = slot >> 7
        low[:, cols] = lo
        high[:, cols] = hi
        picked = jnp.zeros((columns, LANES), F32)
        for tile in range(tiles):
            found = jnp.take_along_axis(values[tile], lo, axis=1, mode="promise_in_bounds")
            picked = jnp.where(hi == tile, found, picked)
        pre = dot(w_diff, own_ref[cols, :], 1, 1) + picked
        sig = jax.nn.sigmoid(pre)
        slope = sig * (1.0 + pre * (1.0 - sig))
        edge[:, cols] = (grad_ref[:, cols].astype(F32) * slope).astype(BF16).astype(F32)

    rows_hi = spread.shape[1]
    lane_ids = lax.broadcasted_iota(jnp.int32, (LANES, points), 0)
    tile_ids = lax.broadcasted_iota(jnp.int32, (rows_hi, points), 0)

    def one_channel(c, _):
        at = pl.ds(c, 1)
        right = jnp.where(lane_ids == low[at, :], 1.0, 0.0).astype(BF16)
        left = jnp.where(tile_ids == high[at, :], edge[at, :], 0.0).astype(BF16)
        spread[c] = dot(left, right, 1, 1)
        return 0

    lax.fori_loop(0, columns, one_channel, 0, unroll=8)

    g = edge[...].astype(BF16)
    own_part = dot(g, own_ref[...], 1, 0)
    nbr_total = jnp.zeros((columns, width), F32)
    for tile in range(tiles):
        got = spread[:, tile, :].astype(BF16)
        nbr_total = nbr_total + dot(got, window_tile(tile), 1, 0)
        given = dot(got, w_nbr, 0, 0)
        block, part = tile // per_block, tile % per_block
        offset = block - REACH
        if offset == 0:
            cols = pl.ds(part * LANES, LANES)
            self_ref[cols, :] = given + dot(edge[:, cols].astype(BF16), w_diff, 0, 0)
        else:
            row = (abs(offset) - 1) * points + part * LANES
            side = ch if offset > 0 else 1 - ch
            contrib[side, pl.ds(row, LANES), :] = given
    keep_ref[...] = contrib[0]
    give_ref[...] = contrib[1].astype(BF16)
    terms_ref[pl.ds(0, columns), :] = own_part
    terms_ref[pl.ds(columns, columns), :] = nbr_total - own_part


def local_math(ch, own, mine, other, w_diff, w_nbr, slot, pick, grad):
    points, width = own.shape
    columns = w_nbr.shape[0]
    tiles = (2 * REACH + 1) * points // LANES
    rows_hi = -(-tiles // 16) * 16
    vmem = pl.BlockSpec(memory_space=pltpu.VMEM)
    return pl.pallas_call(
        local_kernel,
        out_shape=(
            jax.ShapeDtypeStruct((REACH * points, width), F32),
            jax.ShapeDtypeStruct((REACH * points, width), BF16),
            jax.ShapeDtypeStruct((points, width), F32),
            jax.ShapeDtypeStruct((2 * columns, width), F32),
        ),
        in_specs=[pl.BlockSpec(memory_space=pltpu.SMEM)] + [vmem] * 8,
        out_specs=(vmem,) * 4,
        scratch_shapes=[
            pltpu.VMEM((tiles, columns, LANES), F32),
            pltpu.VMEM((columns, points), jnp.int32),
            pltpu.VMEM((columns, points), jnp.int32),
            pltpu.VMEM((columns, points), F32),
            pltpu.VMEM((columns, rows_hi, LANES), F32),
            pltpu.VMEM((2, REACH * points, width), F32),
        ],
        name="local_math",
    )(ch, own, mine, other, w_diff, w_nbr, slot, pick, grad)


def split_shift(x, distance):
    blocks = lax.axis_size("blk")
    cores = lax.axis_size("ch")
    route = [
        (cores * i + c, cores * ((i + (distance if c == 0 else -distance)) % blocks) + c)
        for i in range(blocks)
        for c in range(cores)
    ]
    return lax.ppermute(x, ("blk", "ch"), route)


def swap(x):
    return lax.ppermute(x, "ch", [(0, 1), (1, 0)])


def on_device(features, out_grad, weight, neighbour_slot, argmax_edge):
    points, in_width = features.shape
    blocks = lax.axis_size("blk")
    w_self = weight[:, :in_width]
    w_nbr = weight[:, in_width:]
    w_diff = (w_self.astype(F32) - w_nbr.astype(F32)).astype(BF16)
    ch = lax.axis_index("ch").astype(jnp.int32).reshape(1)

    mine = jnp.concatenate([split_shift(features, d) for d in range(1, REACH + 1)], axis=0)
    other = swap(mine)
    keep, give, own_rows, terms = local_math(
        ch, features, mine, other, w_diff, w_nbr, neighbour_slot.T, argmax_edge.T, out_grad.T
    )

    both = (keep + swap(give).astype(F32)).astype(BF16).reshape(REACH, points, in_width)
    flat = terms.astype(BF16)
    arrived = []
    for d in range(1, REACH + 1):
        load = jnp.concatenate([both[d - 1], flat], axis=0) if d < REACH else both[d - 1]
        arrived.append(split_shift(load, d))
    for part in arrived:
        own_rows = own_rows + part[:points].astype(F32)
    for part in arrived[:-1]:
        terms = terms + part[points:].astype(F32)
    distance = REACH
    while distance < blocks:
        terms = terms + split_shift(terms, distance)
        distance *= 2
    feature_grad = own_rows + swap(own_rows)
    total_points = points * blocks
    columns = weight.shape[0]
    weight_grad = jnp.concatenate([terms[:columns], terms[columns:]], axis=1)
    return (feature_grad, weight_grad * total_points ** (-0.5))


def solution(mesh):
    return jax.shard_map(
        on_device,
        mesh=mesh,
        in_specs=(P("blk", None), P("blk", "ch"), P("ch", None), P("blk", None), P("blk", "ch")),
        out_specs=(P("blk", None), P("ch", None)),
        check_vma=False,
    )
```
